768 devices in a mesh: dp: 32 (over y, z_lo), tensor: 24 (over z_hi, x, core).
Axes of the slice: x: 4, y: 8, z: 12 (z_hi: 3, z_lo: 4; z = z_hi * 4 + z_lo), core: 2. Of those that a mesh axis runs over, the one named last changes fastest.
Arguments:
- activations: bfloat16 [16384, 6144], P('dp', 'tensor'), may hold values from -6 to 6
- cotangent: bfloat16 [16384, 5120], P('dp'), may hold values from -0.046875 to 0.046875
- master: float32 [5120, 6144], P('dp', 'tensor'), may hold values from -0.078125 to 0.078125
- moment_one: float32 [5120, 6144], P('dp', 'tensor'), may hold values from -0.3 to 0.3
- moment_two: float32 [5120, 6144], P('dp', 'tensor'), may hold values from 0.0002 to 0.002
- prompts: bfloat16 [6144, 6144], P('dp', 'tensor'), may hold values from -6 to 6
Outputs:
- new_master: float32 [5120, 6144], P('dp', 'tensor')
- new_moment_one: float32 [5120, 6144], P('dp', 'tensor')
- new_moment_two: float32 [5120, 6144], P('dp', 'tensor')
- projected: bfloat16 [6144, 5120], P(('dp', 'tensor'))
The draws below stay inside these ranges and needn't reach their ends.
All inputs are finite; a program needn't handle non-finite values.
Results may differ from the reference program's by a relative error of at most 0.03.
Values may be sent and summed in bfloat16 or wider, within the bound.
A program may use at most 32 MiB of HBM per device.

```python
import math
import jax
import jax.numpy as jnp
from jax import lax

D = 5120
TOK_DEV = 512
IN = 6144
TOKENS = 16384
PROMPTS = 6144
N_DP = 32
N_TENSOR = 24


def with_spikes(entries, own_key, source, target, parts, factor):
    def block_of(dim):
        return (jnp.arange(entries.shape[dim]) // (entries.shape[dim] // parts)).reshape((-1,) + (1,) * (entries.ndim - 1 - dim))

    one_side = jax.random.permutation(own_key, parts)[block_of(target)]
    other_side = (block_of(target) + parts // 2) % parts
    return jnp.where((block_of(source) == one_side) | (block_of(source) == other_side), factor * entries, entries)


def block_scale(own_key, shape, cuts, smallest, largest):
    def one(dim, parts):
        heights = jax.random.uniform(jax.random.fold_in(jax.random.fold_in(own_key, 6), dim), (parts,), jnp.float32, smallest / len(cuts), largest / len(cuts))
        return jnp.repeat(jnp.exp(heights), shape[dim] // parts).reshape((-1,) + (1,) * (len(shape) - dim - 1))

    factor_of = one(*cuts[0])
    for cut in cuts[1:]:
        factor_of = factor_of * one(*cut)
    return factor_of


def centred(rng, extent, spread, limit, shards=(), held_as=jnp.bfloat16):
    factor_of = block_scale(rng, extent, shards, -0.22, 0.18) if shards else 1.0
    entries = jax.random.normal(rng, extent, jnp.float32) * spread * factor_of
    return jnp.minimum(jnp.maximum(entries, -limit), limit).astype(held_as)


def heavy_noise(rng, shape, scale, most, shards, heavy, held_as=jnp.bfloat16):
    values = scale * jax.random.normal(rng, shape, jnp.float32)
    if shards:
        values = values * block_scale(rng, shape, shards, -0.22, 0.18)
    return jnp.clip(with_spikes(values, jax.random.fold_in(rng, 3), *heavy), -most, most).astype(held_as)


def setup_inputs(seed: int = 0) -> dict:
    seeds = jax.random.split(jax.random.key(seed), 7)
    activations = centred(seeds[0], (TOKENS, IN), 1.0, 6.0, ((0, 32), (1, 24)))
    cotangent = heavy_noise(seeds[1], (TOKENS, D), (TOKENS ** -0.5), 0.046875, ((0, 32),), (0, 1, 32, 2.75))
    master = centred(seeds[2], (D, IN), IN ** -0.5, 0.078125, ((0, 32), (1, 24)), jnp.float32)
    moment_one = centred(seeds[3], (D, IN), 0.05, 0.3, ((0, 32), (1, 24)), jnp.float32)
    moment_two = jnp.clip(jnp.exp(math.log(0.002) - 2.3025852 * jax.random.uniform(seeds[4], (D, IN), jnp.float32) ** block_scale(seeds[4], (D, IN), ((0, 32), (1, 24)), -0.2, 0.2)), 0.0002, 0.002)
    prompts = centred(seeds[5], (PROMPTS, IN), 1.0, 6.0, ((0, 32), (1, 24)))
    return dict(activations=activations, cotangent=cotangent, master=master, moment_one=moment_one, moment_two=moment_two, prompts=prompts)


def reference(activations, cotangent, master, moment_one, moment_two, prompts):
    act_blocks = activations.reshape(N_DP, TOK_DEV, IN)
    cot_blocks = cotangent.reshape(N_DP, TOK_DEV, D)

    def add_block(total, pair):
        acts, cots = pair
        term = lax.dot_general(cots, acts, (((0,), (0,)), ((), ())), preferred_element_type=jnp.float32)
        rounded = lax.optimization_barrier(term.astype(jnp.bfloat16))
        return (total + rounded.astype(jnp.float32), None)
    grad, _ = lax.scan(add_block, jnp.zeros((D, IN), jnp.float32), (act_blocks, cot_blocks))
    new_one = 0.9 * moment_one + 0.1 * grad
    new_two = 0.999 * moment_two + 0.001 * grad * grad
    first = new_one / (1.0 - 0.9 ** 50)
    second = new_two / (1.0 - 0.999 ** 50)
    new_master = master - 0.003 * (first / (jnp.sqrt(second) + 1e-08) + 0.01 * master)
    rollout_weight = new_master.astype(jnp.bfloat16)
    width = IN // N_TENSOR
    prompt_blocks = prompts.reshape(PROMPTS, N_TENSOR, width).transpose(1, 0, 2)
    weight_blocks = rollout_weight.reshape(D, N_TENSOR, width).transpose(1, 0, 2)

    def add_part(total, pair):
        rows, weights = pair
        part = lax.dot_general(rows, weights, (((1,), (1,)), ((), ())), preferred_element_type=jnp.float32)
        rounded = lax.optimization_barrier(part.astype(jnp.bfloat16))
        return (total + rounded.astype(jnp.float32), None)
    summed, _ = lax.scan(add_part, jnp.zeros((PROMPTS, D), jnp.float32), (prompt_blocks, weight_blocks))
    return (new_master, new_one, new_two, summed.astype(jnp.bfloat16))
```

```python
import functools

import jax
import jax.numpy as jnp
from jax import lax
from jax.experimental import pallas as pl
from jax.experimental.pallas import tpu as pltpu
from jax.sharding import Mesh
from jax.sharding import PartitionSpec as P

AXES = ("y", "zl", "zh", "x", "c")
NY, NL, NH, NX, NC = 8, 4, 3, 4, 2
NZ = NL * NH
BF = jnp.bfloat16
F32 = jnp.float32

ROWS = 160
COLS = 256
OUTS = NY * ROWS // 2
SUB = NH * 16


def kernel(
    act_hbm, cot_hbm, master_hbm, one_hbm, two_hbm, prompts_hbm,
    master_out, one_out, two_out, proj_out,
    act, cot, state, new_state, own_prompts, prompts, terms, ring, ring_z, weight,
    own_part, core_out, core_in, x_out, x_in, z_out, z_in, half_sum, half_in, proj,
    load_sem, cot_sem, store_sem, p_send, p_recv, y_send, y_recv, z_send, z_recv,
    w_send, w_recv, c_send, c_recv, x_send, x_recv, f_send, f_recv, h_send, h_recv,
):
    y, zl, zh, x, c = (lax.axis_index(axis) for axis in AXES)
    sent = []

    def go(src, dst, send_sem, recv_sem, to):
        copy = pltpu.make_async_remote_copy(
            src_ref=src, dst_ref=dst, send_sem=send_sem, recv_sem=recv_sem,
            device_id=to, device_id_type=pl.DeviceIdType.MESH,
        )
        copy.start()
        return copy

    def send(src, dst, send_sem, recv_sem, to):
        sent.append(go(src, dst, send_sem, recv_sem, to))

    def arrived(dst, recv_sem):
        pltpu.make_async_copy(dst, dst, recv_sem).wait()

    def cot_copy(r):
        first = pl.multiple_of(lax.rem(y + r, NY) * 640, 640)
        return pltpu.make_async_copy(cot_hbm.at[:, pl.ds(first, 640)], cot.at[r], cot_sem.at[r])

    act_copy = pltpu.make_async_copy(act_hbm, act, load_sem.at[0])
    act_copy.start()
    order = (4, 3, 5, 2, 6, 1, 7, 0)
    for r in order[:3]:
        cot_copy(r).start()
    prompt_copies = [
        pltpu.make_async_copy(prompts_hbm.at[:, i], own_prompts.at[i], load_sem.at[1 + i]) for i in range(NX)
    ]
    for copy in prompt_copies:
        copy.start()
    for r in order[3:]:
        cot_copy(r).start()
    state_copies = [
        pltpu.make_async_copy(ref, state.at[i], load_sem.at[5 + i])
        for i, ref in enumerate((master_hbm, one_hbm, two_hbm))
    ]
    for copy in state_copies:
        copy.start()

    barrier = pltpu.get_barrier_semaphore()
    peers = [{"y": lax.rem(y + 1, NY)}, {"y": lax.rem(y + NY - 1, NY)}]
    peers += [{"x": lax.rem(x + 1, NX)}, {"x": lax.rem(x + NX - 1, NX)}, {"c": 1 - c}]
    for dh in range(NH):
        for dl in range(NL):
            if dh or dl:
                peers.append({"zh": lax.rem(zh + dh, NH), "zl": lax.rem(zl + dl, NL)})
    for peer in peers:
        pl.semaphore_signal(barrier, inc=1, device_id=peer, device_id_type=pl.DeviceIdType.MESH)

    def term(r):
        cot_copy(r).wait()
        for b in range(5):
            block = lax.dot_general(
                cot[r, :, b * 128 : (b + 1) * 128], act[...],
                (((0,), (0,)), ((), ())), preferred_element_type=F32,
            )
            terms[r, b * 128 : (b + 1) * 128, :] = block.astype(BF)

    act_copy.wait()
    term(4)
    for copy in prompt_copies:
        copy.wait()
    pl.semaphore_wait(barrier, len(peers))

    step = (1, NY - 1)

    def z_rel(i):
        return lax.rem(zl + 1 + i, NL)

    def rows_of(i):
        return pl.ds(pl.multiple_of(z_rel(i) * ROWS, ROWS), ROWS)

    for k in (4, 3, 2, 1):
        if k < 4:
            term(k)
            term(NY - k)
        for i in range(NL):
            rows = rows_of(i)
            for d in range(2):
                r = (step[d] * k) % NY
                half = slice(d * 128, (d + 1) * 128)
                cols = half if k == 4 else slice(0, COLS)
                if k < 4:
                    got = half if k == 3 else slice(0, COLS)
                    arrived(ring.at[d, k, i, :, got], y_recv.at[d, k, i])
                    total = terms[r, rows, got].astype(F32) + ring[d, k, i, :, got].astype(F32)
                    terms[r, rows, got] = total.astype(BF)
                send(
                    terms.at[r, rows, cols], ring.at[d, k - 1, i, :, cols],
                    y_send.at[d, k, i], y_recv.at[d, k - 1, i], {"y": lax.rem(y + step[d], NY)},
                )
        if k == 4:
            for dl in range(1, NL):
                send(
                    own_prompts, prompts.at[zl], p_send.at[dl - 1], p_recv.at[dl - 1],
                    {"zl": lax.rem(zl + dl, NL)},
                )
            prompts[zl] = own_prompts[...]
    term(0)

    for i in range(NL):
        rows = rows_of(i)
        for d in range(2):
            arrived(ring.at[d, 0, i], y_recv.at[d, 0, i])
        total = terms[0, rows, :].astype(F32) + ring[0, 0, i].astype(F32) + ring[1, 0, i].astype(F32)
        if i < NL - 1:
            terms[0, rows, :] = total.astype(BF)
            send(
                terms.at[0, rows, :], ring_z.at[i], z_send.at[i], z_recv.at[i],
                {"zl": lax.rem(zl + 1 + i, NL)},
            )
    grad = total
    for copy in state_copies:
        copy.wait()
    for i in range(NL - 1):
        arrived(ring_z.at[i], z_recv.at[i])
        grad = grad + ring_z[i].astype(F32)

    new_one = 0.9 * state[1] + 0.1 * grad
    new_two = 0.999 * state[2] + 0.001 * grad * grad
    first = new_one / (1.0 - 0.9**50)
    second = new_two / (1.0 - 0.999**50)
    old = state[0]
    new_master = old - 0.003 * (first / (jnp.sqrt(second) + 1e-08) + 0.01 * old)
    weight[y] = new_master.astype(BF)
    new_state[0] = new_master
    new_state[1] = new_one
    new_state[2] = new_two

    def piece(n):
        return pl.ds((n // 2) * 80, 80), pl.ds((n % 2) * 128, 128)

    for s in range(1, 5):
        for n in range(4):
            for d in range(2):
                if s == 4 and n // 2 != d:
                    continue
                origin = lax.rem(y + (NY - step[d]) * (s - 1), NY)
                part = weight.at[(origin, *piece(n))]
                if s > 1:
                    arrived(part, w_recv.at[d, s - 2, n])
                send(
                    part, part, w_send.at[d, s - 1, n], w_recv.at[d, s - 1, n],
                    {"y": lax.rem(y + step[d], NY)},
                )
        if s == 1:
            stores = [
                pltpu.make_async_copy(new_state.at[i], ref, store_sem.at[i])
                for i, ref in enumerate((master_out, one_out, two_out))
            ]
            for copy in stores:
                copy.start()
            for dl in range(1, NL):
                arrived(prompts.at[0], p_recv.at[dl - 1])
    for s in (3, 4):
        for n in range(4):
            for d in range(2):
                if s == 4 and n // 2 != d:
                    continue
                if s == 3 and n // 2 == d:
                    continue
                origin = lax.rem(y + (NY - step[d]) * s, NY)
                arrived(weight.at[(origin, *piece(n))], w_recv.at[d, s - 1, n])

    x_order = (2, 1, 3, 0)

    def project(i, core):
        x_to = lax.rem(x + x_order[i], NX)
        lhs = jnp.concatenate([prompts[n, x_to].reshape(SUB, COLS) for n in range(NL)], axis=0)
        rhs = weight[pl.ds(4 * core, 4)].reshape(OUTS, COLS)
        return lax.dot_general(lhs, rhs, (((1,), (1,)), ((), ())), preferred_element_type=F32)

    for i in range(NX):
        core_out[i] = project(i, 1 - c).astype(BF)
        send(core_out.at[i], core_in.at[i], c_send.at[i], c_recv.at[i], {"c": 1 - c})
        own_part[i] = project(i, c)

    x_dir = (1, NX - 1)

    def part_sum(i, n):
        rows = slice(n * SUB, (n + 1) * SUB)
        return own_part[i, rows, :] + core_in[i, rows, :].astype(F32)

    def x_send_to(d, i, n, k):
        send(
            x_out.at[i, n], x_in.at[d, k, n], x_send.at[d, k, n], x_recv.at[d, k, n],
            {"x": lax.rem(x + x_dir[d], NX)},
        )

    def far(d, n):
        x_out[0, n] = part_sum(0, n).astype(BF)
        x_send_to(d, 0, n, 1)

    def near(d, n):
        total = part_sum(1 + d, n)
        if n // 2 == d:
            arrived(x_in.at[d, 1, n], x_recv.at[d, 1, n])
            total = total + x_in[d, 1, n].astype(F32)
        x_out[1 + d, n] = total.astype(BF)
        x_send_to(d, 1 + d, n, 0)

    arrived(core_in.at[0], c_recv.at[0])
    far(0, 0)
    far(1, 2)
    arrived(core_in.at[1], c_recv.at[1])
    near(0, 2)
    arrived(core_in.at[2], c_recv.at[2])
    near(1, 0)
    far(0, 1)
    far(1, 3)
    near(0, 0)
    near(1, 2)
    near(0, 3)
    near(1, 1)
    near(0, 1)
    near(1, 3)
    arrived(core_in.at[3], c_recv.at[3])

    me = zh * NL + zl
    for n in (0, 2, 1, 3):
        total = part_sum(3, n)
        for d in range(2):
            arrived(x_in.at[d, 0, n], x_recv.at[d, 0, n])
            total = total + x_in[d, 0, n].astype(F32)
        z_out[n] = total.astype(BF).reshape(NH, 16, OUTS)
        for h in range(NH):
            to = h * NL + n

            @pl.when(me != to)
            def _():
                go(z_out.at[n, h], z_in.at[me], f_send.at[to], f_recv.at[me], {"zh": h, "zl": n})

    z_in[me] = z_out[zl, zh]
    for at in range(NZ):

        @pl.when(me != at)
        def _():
            arrived(z_in.at[at], f_recv.at[at])

    for n in range(NL):
        half_sum[n] = z_in[n].astype(F32) + z_in[NL + n].astype(F32) + z_in[2 * NL + n].astype(F32)
    theirs = pl.ds(pl.multiple_of(8 * (1 - c), 8), 8)
    mine = pl.ds(pl.multiple_of(8 * c, 8), 8)
    send(half_sum.at[:, theirs, :], half_in, h_send.at[0], h_recv.at[0], {"c": 1 - c})

    def laid_out(read):
        parts = [read(n) for n in range(NL)]
        return jnp.concatenate(
            [parts[n][:, j * ROWS : (j + 1) * ROWS] for j in range(4) for n in range(NL)], axis=1
        ).astype(BF)

    own_at = pl.ds(pl.multiple_of(c * 2560, 2560), 2560)
    proj[:, own_at] = laid_out(lambda n: half_sum[n, mine, :])
    arrived(half_in, h_recv.at[0])
    other_at = pl.ds(pl.multiple_of((1 - c) * 2560, 2560), 2560)
    proj[:, other_at] = laid_out(lambda n: half_in[n])
    last = pltpu.make_async_copy(proj, proj_out, store_sem.at[3])
    last.start()

    for copy in sent:
        copy.wait_send()
    for to in range(NZ):

        @pl.when(me != to)
        def _():
            pltpu.make_async_copy(z_in.at[0], z_in.at[0], f_send.at[to]).wait()

    for copy in stores:
        copy.wait()
    last.wait()


def local(activations, cotangent, master, moment_one, moment_two, prompts):
    any_space = pl.BlockSpec(memory_space=pl.ANY)
    dma = pltpu.SemaphoreType.DMA
    weight_shape = jax.ShapeDtypeStruct((ROWS, COLS), F32)
    return pl.pallas_call(
        kernel,
        out_shape=(weight_shape, weight_shape, weight_shape, jax.ShapeDtypeStruct((8, 5120), BF)),
        in_specs=[any_space] * 6,
        out_specs=[any_space] * 4,
        scratch_shapes=[
            pltpu.VMEM((512, COLS), BF),
            pltpu.VMEM((NY, 512, 640), BF),
            pltpu.VMEM((3, ROWS, COLS), F32),
            pltpu.VMEM((3, ROWS, COLS), F32),
            pltpu.VMEM((NX, NH, 16, COLS), BF),
            pltpu.VMEM((NL, NX, NH, 16, COLS), BF),
            pltpu.VMEM((NY, 640, COLS), BF),
            pltpu.VMEM((2, 4, NL, ROWS, COLS), BF),
            pltpu.VMEM((NL - 1, ROWS, COLS), BF),
            pltpu.VMEM((NY, ROWS, COLS), BF),
            pltpu.VMEM((NX, NL * SUB, OUTS), F32),
            pltpu.VMEM((NX, NL * SUB, OUTS), BF),
            pltpu.VMEM((NX, NL * SUB, OUTS), BF),
            pltpu.VMEM((3, NL, SUB, OUTS), BF),
            pltpu.VMEM((2, 2, NL, SUB, OUTS), BF),
            pltpu.VMEM((NL, NH, 16, OUTS), BF),
            pltpu.VMEM((NZ, 16, OUTS), BF),
            pltpu.VMEM((NL, 16, OUTS), F32),
            pltpu.VMEM((NL, 8, OUTS), F32),
            pltpu.VMEM((8, 5120), BF),
            dma((8,)), dma((NY,)), dma((4,)),
            dma((3,)), dma((3,)),
            dma((2, 5, NL)), dma((2, 4, NL)),
            dma((3,)), dma((3,)),
            dma((2, 4, 4)), dma((2, 4, 4)),
            dma((NX,)), dma((NX,)),
            dma((2, 2, NL)), dma((2, 2, NL)),
            dma((NZ,)), dma((NZ,)),
            dma((1,)), dma((1,)),
        ],
        compiler_params=pltpu.CompilerParams(collective_id=0, has_side_effects=True),
        name="step",
    )(activations, cotangent, master, moment_one, moment_two, prompts.reshape(NH, NX, 16, COLS))


def solution(mesh):
    torus = Mesh(mesh.devices.reshape(NY, NL, NH, NX, NC), AXES)
    dp, tensor = ("y", "zl"), ("zh", "x", "c")
    both = P(dp, tensor)
    in_specs = (both, P(dp, None), both, both, both, both)
    out_specs = (both, both, both, P(dp + tensor, None))
    return jax.shard_map(local, mesh=torus, in_specs=in_specs, out_specs=out_specs, check_vma=False)
```

```python
import jax
import jax.numpy as jnp
from jax import lax
from jax.experimental import pallas as pl
from jax.experimental.pallas import tpu as pltpu
from jax.sharding import Mesh
from jax.sharding import PartitionSpec as P

AXES = ("y", "zl", "zh", "x", "c")
NY, NL, NH, NX, NC = 8, 4, 3, 4, 2
NZ = NL * NH
BF = jnp.bfloat16
F32 = jnp.float32

ROWS = 160
FIRST_Y = 112
REST = ROWS - FIRST_Y
COLS = 256
OUTS = 4 * ROWS
SUB = NH * 16
PLACE = (0, 1, 7, 2, 6, 3, 5, 4)
SLOT = tuple(PLACE.index(r) for r in range(NY))
MESH = pl.DeviceIdType.MESH


def kernel(
    act_hbm, cot_hbm, master_hbm, one_hbm, two_hbm, prompts_hbm,
    state_out, proj_out,
    act, cot, state, new_state, own_prompts, prompts, terms, ring, ring_z, rest_z, rest_y, rest_sum,
    weight, own_part, core_out, core_in, x_out, x_in, z_out, z_in, half_sum, half_in, proj,
    load_sem, cot_sem, store_sem, p_send, p_recv, y_send, y_recv, z_send, z_recv,
    rz_send, rz_recv, ry_send, ry_recv,
    w_send, w_recv, c_send, c_recv, x_send, x_recv, f_send, f_recv, h_send, h_recv,
):
    y, zl, zh, x, c = (lax.axis_index(axis) for axis in AXES)
    sent = []

    def go(src, dst, send_sem, recv_sem, to):
        copy = pltpu.make_async_remote_copy(
            src_ref=src, dst_ref=dst, send_sem=send_sem, recv_sem=recv_sem,
            device_id=to, device_id_type=MESH,
        )
        copy.start()
        return copy

    def send(src, dst, send_sem, recv_sem, to):
        sent.append(go(src, dst, send_sem, recv_sem, to))

    def arrived(dst, recv_sem):
        pltpu.make_async_copy(dst, dst, recv_sem).wait()

    def cot_copy(r):
        first = pl.multiple_of(lax.rem(y + r, NY) * 640, 640)
        return pltpu.make_async_copy(cot_hbm.at[:, pl.ds(first, 640)], cot.at[r], cot_sem.at[r])

    act_copy = pltpu.make_async_copy(act_hbm, act, load_sem.at[0])
    act_copy.start()
    for r in (4, 3, 5, 2, 6, 1, 7, 0):
        cot_copy(r).start()
    prompt_copies = [
        pltpu.make_async_copy(prompts_hbm.at[:, i], own_prompts.at[i], load_sem.at[1 + i]) for i in range(NX)
    ]
    state_copies = [
        pltpu.make_async_copy(ref, state.at[i], load_sem.at[5 + i])
        for i, ref in enumerate((master_hbm, one_hbm, two_hbm))
    ]
    for copy in prompt_copies + state_copies:
        copy.start()

    barrier = pltpu.get_barrier_semaphore()
    peers = [{"y": lax.rem(y + i, NY)} for i in range(1, NY)]
    peers += [{"zl": lax.rem(zl + i, NL)} for i in range(1, NL)]
    peers += [{"x": lax.rem(x + 1, NX)}, {"x": lax.rem(x + NX - 1, NX)}, {"c": 1 - c}]
    for peer in peers:
        pl.semaphore_signal(barrier, inc=1, device_id=peer, device_id_type=MESH)
    me = zh * NL + zl
    own_half = zl // 2 == c
    for h in range(NH):
        for n in range(NL):

            @pl.when(jnp.logical_or(me != h * NL + n, jnp.logical_not(own_half)))
            def _():
                pl.semaphore_signal(
                    barrier, inc=1, device_id={"zh": h, "zl": n, "c": zl // 2}, device_id_type=MESH
                )

    def term(r):
        cot_copy(r).wait()
        for b in range(5):
            block = lax.dot_general(
                cot[r, :, b * 128 : (b + 1) * 128], act[...],
                (((0,), (0,)), ((), ())), preferred_element_type=F32,
            )
            terms[r, b * 128 : (b + 1) * 128, :] = block.astype(BF)

    def z_rel(i):
        return lax.rem(zl + 1 + i, NL)

    def rows_of(i):
        return pl.ds(pl.multiple_of(z_rel(i) * ROWS, ROWS), FIRST_Y)

    def rest_of(i):
        return pl.ds(pl.multiple_of(z_rel(i) * ROWS + FIRST_Y, 16), REST)

    def rest_over_z(r):
        for i in range(NL - 1):
            send(
                terms.at[r, rest_of(i), :], rest_z.at[r, i], rz_send.at[r, i], rz_recv.at[r, i], {"zl": z_rel(i)}
            )

    def rest_total(r):
        total = terms[r, rest_of(NL - 1), :].astype(F32)
        for i in range(NL - 1):
            arrived(rest_z.at[r, i], rz_recv.at[r, i])
            total = total + rest_z[r, i].astype(F32)
        return total

    def rest_over_y(r):
        rest_sum[r] = rest_total(r).astype(BF)
        send(rest_sum.at[r], rest_y.at[r], ry_send.at[r], ry_recv.at[r], {"y": lax.rem(y + r, NY)})

    act_copy.wait()
    term(4)
    pl.semaphore_wait(barrier, len(peers) + 12 - own_half.astype(jnp.int32))

    step = (1, NY - 1)

    def chain(k):
        for i in range(NL):
            rows = rows_of(i)
            for d in range(2):
                r = (step[d] * k) % NY
                half = slice(d * 128, (d + 1) * 128)
                cols = half if k == 4 else slice(0, COLS)
                if k < 4:
                    got = half if k == 3 else slice(0, COLS)
                    arrived(ring.at[d, k, i, :, got], y_recv.at[d, k, i])
                    total = terms[r, rows, got].astype(F32) + ring[d, k, i, :, got].astype(F32)
                    terms[r, rows, got] = total.astype(BF)
                send(
                    terms.at[r, rows, cols], ring.at[d, k - 1, i, :, cols],
                    y_send.at[d, k, i], y_recv.at[d, k - 1, i], {"y": lax.rem(y + step[d], NY)},
                )

    chain(4)
    rest_over_z(4)
    for r in (3, 5):
        term(r)
        rest_over_z(r)
    chain(3)
    for r in (2, 6):
        term(r)
        rest_over_z(r)
    rest_over_y(4)
    chain(2)
    for r in (1, 7, 0):
        term(r)
        rest_over_z(r)
    for r in (3, 5):
        rest_over_y(r)
    chain(1)
    for r in (2, 6, 1, 7):
        rest_over_y(r)

    for i in range(NL):
        rows = rows_of(i)
        for d in range(2):
            arrived(ring.at[d, 0, i], y_recv.at[d, 0, i])
        total = terms[0, rows, :].astype(F32) + ring[0, 0, i].astype(F32) + ring[1, 0, i].astype(F32)
        if i < NL - 1:
            terms[0, rows, :] = total.astype(BF)
            send(terms.at[0, rows, :], ring_z.at[i], z_send.at[i], z_recv.at[i], {"zl": z_rel(i)})
    for copy in prompt_copies:
        copy.wait()
    for i in range(NL - 1):
        send(own_prompts, prompts.at[zl], p_send.at[i], p_recv.at[i], {"zl": z_rel(i)})
    prompts[zl] = own_prompts[...]
    for copy in state_copies:
        copy.wait()

    def update(at, grad):
        new_one = 0.9 * state[1, at] + 0.1 * grad
        new_two = 0.999 * state[2, at] + 0.001 * grad * grad
        first = new_one / (1.0 - 0.9**50)
        second = new_two / (1.0 - 0.999**50)
        old = state[0, at]
        new_master = old - 0.003 * (first / (jnp.sqrt(second) + 1e-08) + 0.01 * old)
        weight[0, at] = new_master.astype(BF)
        new_state[0, at] = new_master
        new_state[1, at] = new_one
        new_state[2, at] = new_two

    grad = rest_total(0)
    for r in (4, 3, 5, 2, 6, 1, 7):
        arrived(rest_y.at[r], ry_recv.at[r])
        grad = grad + rest_y[r].astype(F32)
    update(slice(FIRST_Y, ROWS), grad)
    grad = total
    for i in range(NL - 1):
        arrived(ring_z.at[i], z_recv.at[i])
        grad = grad + ring_z[i].astype(F32)
    update(slice(0, FIRST_Y), grad)

    def piece(place, n):
        return weight.at[place, pl.ds((n // 2) * 80, 80), pl.ds((n % 2) * 128, 128)]

    def held(d, s):
        return SLOT[(NY - step[d] * s) % NY]

    def pass_on(s, n, d, hops=1):
        send(
            piece(held(d, s - 1), n), piece(held(d, s - 2 + hops + 1), n), w_send.at[d, s - 2 + hops, n],
            w_recv.at[d, s - 2 + hops, n], {"y": lax.rem(y + hops * step[d], NY)},
        )

    def landed(s, n, d):
        arrived(piece(held(d, s), n), w_recv.at[d, s - 1, n])

    x_order = (2, 1, 3, 0)

    def project(g, i, core):
        x_to = lax.rem(x + x_order[i], NX)
        lhs = jnp.concatenate([prompts[2 * core + n, x_to].reshape(SUB, COLS) for n in range(2)], axis=0)
        rhs = weight[4 * g : 4 * g + 4].reshape(OUTS, COLS)
        return lax.dot_general(lhs, rhs, (((1,), (1,)), ((), ())), preferred_element_type=F32)

    def project_all(g):
        for i in range(NX):
            core_out[g, i] = project(g, i, 1 - c).astype(BF)
            send(core_out.at[g, i], core_in.at[g, i], c_send.at[g, i], c_recv.at[g, i], {"c": 1 - c})
        for i in range(NX):
            own_part[g, i] = project(g, i, c)

    x_dir = (1, NX - 1)

    def part_sum(g, i, n):
        rows = slice(n * SUB, (n + 1) * SUB)
        return own_part[g, i, rows, :] + core_in[g, i, rows, :].astype(F32)

    def x_send_to(g, d, i, n, k):
        send(
            x_out.at[g, i, n], x_in.at[g, d, k, n], x_send.at[g, d, k, n], x_recv.at[g, d, k, n],
            {"x": lax.rem(x + x_dir[d], NX)},
        )

    def far(g):
        arrived(core_in.at[g, 0], c_recv.at[g, 0])
        for d in range(2):
            x_out[g, 0, d] = part_sum(g, 0, d).astype(BF)
            x_send_to(g, d, 0, d, 1)

    def near(g, d, n):
        total = part_sum(g, 1 + d, n)
        if n == d:
            arrived(x_in.at[g, d, 1, n], x_recv.at[g, d, 1, n])
            total = total + x_in[g, d, 1, n].astype(F32)
        x_out[g, 1 + d, n] = total.astype(BF)
        x_send_to(g, d, 1 + d, n, 0)

    def x_first(g):
        far(g)
        for d in range(2):
            arrived(core_in.at[g, 1 + d], c_recv.at[g, 1 + d])
            near(g, d, 1 - d)

    def x_second(g):
        for d in range(2):
            near(g, d, d)
        arrived(core_in.at[g, 3], c_recv.at[g, 3])

    def over_z(g):
        for n in range(2):
            total = part_sum(g, 3, n)
            for d in range(2):
                arrived(x_in.at[g, d, 0, n], x_recv.at[g, d, 0, n])
                total = total + x_in[g, d, 0, n].astype(F32)
            z_out[g, n] = total.astype(BF).reshape(NH, 16, OUTS)
            for h in range(NH):
                to = h * NL + 2 * c + n
                stays = jnp.logical_and(me == to, c == g)

                @pl.when(stays)
                def _():
                    z_in[me] = z_out[g, n, h]

                @pl.when(jnp.logical_not(stays))
                def _():
                    go(
                        z_out.at[g, n, h], z_in.at[me], f_send.at[g, n, h], f_recv.at[me],
                        {"zh": h, "zl": 2 * c + n, "c": g},
                    )

    for n in range(4):
        for d in range(2):
            pass_on(1, n, d)
    state_copy = pltpu.make_async_copy(new_state, state_out, store_sem.at[0])
    state_copy.start()
    for n in range(4):
        for d in range(2):
            landed(1, n, d)
            pass_on(2, n, d)
    for n in range(4):
        for d in range(2):
            landed(2, n, d)
            if n // 2 == d:
                pass_on(3, n, d, 2)
            pass_on(3, n, d)
    for i in range(NL - 1):
        arrived(prompts.at[0], p_recv.at[i])
    project_all(0)
    x_first(0)
    for n in range(4):
        for d in range(2):
            landed(3, n, d)
            if n // 2 == d:
                landed(4, n, d)
    project_all(1)
    x_second(0)
    x_first(1)
    over_z(0)
    x_second(1)
    over_z(1)

    for at in range(NZ):

        @pl.when(jnp.logical_or(me != at, jnp.logical_not(own_half)))
        def _():
            arrived(z_in.at[at], f_recv.at[at])

    for n in range(NL):
        half_sum[n] = z_in[n].astype(F32) + z_in[NL + n].astype(F32) + z_in[2 * NL + n].astype(F32)
    theirs = pl.ds(pl.multiple_of(8 * (1 - c), 8), 8)
    mine = pl.ds(pl.multiple_of(8 * c, 8), 8)
    send(half_sum.at[:, theirs, :], half_in, h_send.at[0], h_recv.at[0], {"c": 1 - c})

    def lay_out(group, read):
        parts = [read(n) for n in range(NL)]
        for j in range(4):
            block = jnp.concatenate([part[:, j * ROWS : (j + 1) * ROWS] for part in parts], axis=1)
            far_y = lax.rem(y + PLACE[j] + group * (PLACE[4 + j] - PLACE[j]), NY)
            proj[:, pl.ds(pl.multiple_of(far_y * 640, 640), 640)] = block.astype(BF)

    lay_out(c, lambda n: half_sum[n, mine, :])
    arrived(half_in, h_recv.at[0])
    lay_out(1 - c, lambda n: half_in[n])
    last = pltpu.make_async_copy(proj, proj_out, store_sem.at[1])
    last.start()

    for copy in sent:
        copy.wait_send()
    for g in range(2):
        for n in range(2):
            for h in range(NH):

                @pl.when(jnp.logical_or(me != h * NL + 2 * c + n, c != g))
                def _():
                    pltpu.make_async_copy(z_out.at[g, n, h], z_out.at[g, n, h], f_send.at[g, n, h]).wait()

    state_copy.wait()
    last.wait()


def hand_on(state, proj, master_out, one_out, two_out, proj_out, held, held_proj, in_sem, out_sem):
    moves = [(proj, held_proj, proj_out)]
    moves += [(state.at[i], held.at[i], ref) for i, ref in enumerate((master_out, one_out, two_out))]
    reads = [pltpu.make_async_copy(src, mid, in_sem.at[i]) for i, (src, mid, _) in enumerate(moves)]
    writes = [pltpu.make_async_copy(mid, dst, out_sem.at[i]) for i, (_, mid, dst) in enumerate(moves)]
    for copy in reads:
        copy.start()
    for read, write in zip(reads, writes):
        read.wait()
        write.start()
    for copy in writes:
        copy.wait()


def local(activations, cotangent, master, moment_one, moment_two, prompts):
    any_space = pl.BlockSpec(memory_space=pl.ANY)
    dma = pltpu.SemaphoreType.DMA
    state, proj = pl.pallas_call(
        kernel,
        out_shape=(jax.ShapeDtypeStruct((3, ROWS, COLS), F32), jax.ShapeDtypeStruct((8, 5120), BF)),
        in_specs=[any_space] * 6,
        out_specs=[any_space] * 2,
        scratch_shapes=[
            pltpu.VMEM((512, COLS), BF),
            pltpu.VMEM((NY, 512, 640), BF),
            pltpu.VMEM((3, ROWS, COLS), F32),
            pltpu.VMEM((3, ROWS, COLS), F32),
            pltpu.VMEM((NX, NH, 16, COLS), BF),
            pltpu.VMEM((NL, NX, NH, 16, COLS), BF),
            pltpu.VMEM((NY, 640, COLS), BF),
            pltpu.VMEM((2, 4, NL, FIRST_Y, COLS), BF),
            pltpu.VMEM((NL - 1, FIRST_Y, COLS), BF),
            pltpu.VMEM((NY, NL - 1, REST, COLS), BF),
            pltpu.VMEM((NY, REST, COLS), BF),
            pltpu.VMEM((NY, REST, COLS), BF),
            pltpu.VMEM((NY, ROWS, COLS), BF),
            pltpu.VMEM((2, NX, 2 * SUB, OUTS), F32),
            pltpu.VMEM((2, NX, 2 * SUB, OUTS), BF),
            pltpu.VMEM((2, NX, 2 * SUB, OUTS), BF),
            pltpu.VMEM((2, 3, 2, SUB, OUTS), BF),
            pltpu.VMEM((2, 2, 2, 2, SUB, OUTS), BF),
            pltpu.VMEM((2, 2, NH, 16, OUTS), BF),
            pltpu.VMEM((NZ, 16, OUTS), BF),
            pltpu.VMEM((NL, 16, OUTS), F32),
            pltpu.VMEM((NL, 8, OUTS), F32),
            pltpu.VMEM((8, 5120), BF),
            dma((8,)), dma((NY,)), dma((2,)),
            dma((3,)), dma((3,)),
            dma((2, 5, NL)), dma((2, 4, NL)),
            dma((3,)), dma((3,)),
            dma((NY, 3)), dma((NY, 3)),
            dma((NY,)), dma((NY,)),
            dma((2, 4, 4)), dma((2, 4, 4)),
            dma((2, NX)), dma((2, NX)),
            dma((2, 2, 2, 2)), dma((2, 2, 2, 2)),
            dma((2, 2, NH)), dma((NZ,)),
            dma((1,)), dma((1,)),
        ],
        compiler_params=pltpu.CompilerParams(collective_id=0, has_side_effects=True),
        name="step",
    )(activations, cotangent, master, moment_one, moment_two, prompts.reshape(NH, NX, 16, COLS))
    weight_shape = jax.ShapeDtypeStruct((ROWS, COLS), F32)
    return pl.pallas_call(
        hand_on,
        out_shape=(weight_shape, weight_shape, weight_shape, jax.ShapeDtypeStruct((8, 5120), BF)),
        in_specs=[any_space] * 2,
        out_specs=[any_space] * 4,
        scratch_shapes=[pltpu.VMEM((3, ROWS, COLS), F32), pltpu.VMEM((8, 5120), BF), dma((4,)), dma((4,))],
        name="hand_on",
    )(state, proj)


def solution(mesh):
    torus = Mesh(mesh.devices.reshape(NY, NL, NH, NX, NC), AXES)
    dp, tensor = ("y", "zl"), ("zh", "x", "c")
    both = P(dp, tensor)
    in_specs = (both, P(dp, None), both, both, both, both)
    out_specs = (both, both, both, P(dp + tensor, None))
    return jax.shard_map(local, mesh=torus, in_specs=in_specs, out_specs=out_specs, check_vma=False)
```

```python
import jax
import jax.numpy as jnp
from jax import lax
from jax.experimental import pallas as pl
from jax.experimental.pallas import tpu as pltpu
from jax.sharding import Mesh
from jax.sharding import PartitionSpec as P

AXES = ("y", "zl", "zh", "x", "c")
NY, NL, NH, NX, NC = 8, 4, 3, 4, 2
NZ = NL * NH
BF = jnp.bfloat16
F32 = jnp.float32

ROWS = 160
FIRST_Y = 112
REST = ROWS - FIRST_Y
HALF = ((0, 64), (64, 48))
COLS = 256
OUTS = 4 * ROWS
SUB = NH * 16
PLACE = (0, 1, 7, 2, 6, 3, 5, 4)
SLOT = tuple(PLACE.index(r) for r in range(NY))
PIECE = ((0, 48), (48, 32), (80, 48), (128, 32))
MESH = pl.DeviceIdType.MESH


def kernel(
    act_hbm, cot_hbm, master_hbm, one_hbm, two_hbm, prompts_hbm,
    state_out, z_in,
    act, cot, state, new_state, own_prompts, prompts, terms, ring, ring_z, rest_z, rest_y, rest_sum,
    weight, own_part, core_out, core_in, x_out, x_in, z_out,
    load_sem, cot_sem, store_sem, p_send, p_recv, y_send, y_recv, z_send, z_recv,
    rz_send, rz_recv, ry_send, ry_recv,
    w_send, w_recv, c_send, c_recv, x_send, x_recv, f_send, f_recv,
    up_edge, up_group, down_edge, down_group,
):
    y, zl, zh, x, c = (lax.axis_index(axis) for axis in AXES)
    sent = []

    def go(src, dst, send_sem, recv_sem, to):
        copy = pltpu.make_async_remote_copy(
            src_ref=src, dst_ref=dst, send_sem=send_sem, recv_sem=recv_sem,
            device_id=to, device_id_type=MESH,
        )
        copy.start()
        return copy

    def send(src, dst, send_sem, recv_sem, to):
        sent.append(go(src, dst, send_sem, recv_sem, to))

    def arrived(dst, recv_sem):
        pltpu.make_async_copy(dst, dst, recv_sem).wait()

    def cot_copy(r):
        first = pl.multiple_of(lax.rem(y + r, NY) * 640, 640)
        return pltpu.make_async_copy(cot_hbm.at[:, pl.ds(first, 640)], cot.at[r], cot_sem.at[r])

    act_copy = pltpu.make_async_copy(act_hbm, act, load_sem.at[0])
    act_copy.start()
    for r in (4, 3, 5, 2, 6, 1, 7, 0):
        cot_copy(r).start()
    prompt_copies = [
        pltpu.make_async_copy(prompts_hbm.at[:, i], own_prompts.at[i], load_sem.at[1 + i]) for i in range(NX)
    ]
    state_copies = [
        pltpu.make_async_copy(ref, state.at[i], load_sem.at[5 + i])
        for i, ref in enumerate((master_hbm, one_hbm, two_hbm))
    ]
    for copy in prompt_copies + state_copies:
        copy.start()

    barrier = pltpu.get_barrier_semaphore()
    peers = [{"y": lax.rem(y + i, NY)} for i in range(1, NY)]
    peers += [{"zl": lax.rem(zl + i, NL)} for i in range(1, NL)]
    peers += [{"x": lax.rem(x + 1, NX)}, {"x": lax.rem(x + NX - 1, NX)}, {"c": 1 - c}]
    for peer in peers:
        pl.semaphore_signal(barrier, inc=1, device_id=peer, device_id_type=MESH)
    me = zh * NL + zl
    lower_edge = jnp.logical_and(zl == 0, zh > 0)
    upper_edge = jnp.logical_and(zl == NL - 1, zh < NH - 1)

    def tell(semaphore, peer):
        pl.semaphore_signal(semaphore, inc=1, device_id=peer, device_id_type=MESH)

    pl.when(lower_edge)(lambda: tell(barrier, {"zh": zh - 1, "zl": NL - 1}))
    pl.when(upper_edge)(lambda: tell(barrier, {"zh": zh + 1, "zl": 0}))

    def at(h, n):
        return jnp.logical_and(zh == h, zl == n)

    def tell_group(semaphore):
        for i in range(1, NL):
            tell(semaphore, {"zl": lax.rem(zl + i, NL)})

    def word_1():
        pl.when(at(0, 3))(lambda: tell(up_edge, {"zh": 1, "zl": 0}))
        pl.when(at(2, 0))(lambda: tell(down_edge, {"zh": 1, "zl": 3}))

    def hear_and_tell_group(h, n, edge, group):
        @pl.when(at(h, n))
        def _():
            pl.semaphore_wait(edge, 1)
            tell_group(group)

    def word_2():
        hear_and_tell_group(1, 0, up_edge, up_group)
        hear_and_tell_group(1, 3, down_edge, down_group)

    def word_3():
        @pl.when(at(1, 3))
        def _():
            pl.semaphore_wait(up_group, 1)
            tell(up_edge, {"zh": 2, "zl": 0})

        @pl.when(at(1, 0))
        def _():
            pl.semaphore_wait(down_group, 1)
            tell(down_edge, {"zh": 0, "zl": 3})

    def word_4():
        hear_and_tell_group(2, 0, up_edge, up_group)
        hear_and_tell_group(0, 3, down_edge, down_group)

    def word_5():
        middle = jnp.logical_and(zh == 1, jnp.logical_or(zl == 1, zl == 2))
        below = jnp.logical_or(middle, jnp.logical_and(zh == 2, zl != 0))
        above = jnp.logical_or(middle, jnp.logical_and(zh == 0, zl != 3))
        pl.when(below)(lambda: pl.semaphore_wait(up_group, 1))
        pl.when(above)(lambda: pl.semaphore_wait(down_group, 1))

    def term(r):
        cot_copy(r).wait()
        for b in range(5):
            block = lax.dot_general(
                cot[r, :, b * 128 : (b + 1) * 128], act[...],
                (((0,), (0,)), ((), ())), preferred_element_type=F32,
            )
            terms[r, b * 128 : (b + 1) * 128, :] = block.astype(BF)

    def z_rel(i):
        return lax.rem(zl + 1 + i, NL)

    def rows_of(i, first=0, size=FIRST_Y):
        return pl.ds(pl.multiple_of(z_rel(i) * ROWS + first, 16), size)

    def rest_of(i):
        return pl.ds(pl.multiple_of(z_rel(i) * ROWS + FIRST_Y, 16), REST)

    def rest_over_z(r):
        for i in range(NL - 1):
            send(
                terms.at[r, rest_of(i), :], rest_z.at[r, i], rz_send.at[r, i], rz_recv.at[r, i], {"zl": z_rel(i)}
            )

    def rest_total(r):
        total = terms[r, rest_of(NL - 1), :].astype(F32)
        for i in range(NL - 1):
            arrived(rest_z.at[r, i], rz_recv.at[r, i])
            total = total + rest_z[r, i].astype(F32)
        return total

    def rest_over_y(r):
        rest_sum[r] = rest_total(r).astype(BF)
        send(rest_sum.at[r], rest_y.at[r], ry_send.at[r], ry_recv.at[r], {"y": lax.rem(y + r, NY)})

    act_copy.wait()
    term(4)
    pl.semaphore_wait(barrier, len(peers) + lower_edge.astype(jnp.int32) + upper_edge.astype(jnp.int32))

    step = (1, NY - 1)

    def chain(k):
        for i in range(NL):
            for d in range(2):
                r = (step[d] * k) % NY
                half = HALF[d]
                if k < 4:
                    first, size = half if k == 3 else (0, FIRST_Y)
                    got, to = rows_of(i, first, size), pl.ds(first, size)
                    arrived(ring.at[d, k, i, to], y_recv.at[d, k, i])
                    total = terms[r, got, :].astype(F32) + ring[d, k, i, to].astype(F32)
                    terms[r, got, :] = total.astype(BF)
                first, size = half if k == 4 else (0, FIRST_Y)
                send(
                    terms.at[r, rows_of(i, first, size), :], ring.at[d, k - 1, i, pl.ds(first, size)],
                    y_send.at[d, k, i], y_recv.at[d, k - 1, i], {"y": lax.rem(y + step[d], NY)},
                )

    chain(4)
    rest_over_z(4)
    for r in (3, 5):
        term(r)
        rest_over_z(r)
    chain(3)
    for r in (2, 6):
        term(r)
        rest_over_z(r)
    rest_over_y(4)
    word_1()
    chain(2)
    for r in (1, 7, 0):
        term(r)
        rest_over_z(r)
    for r in (3, 5):
        rest_over_y(r)
    chain(1)
    for r in (2, 6, 1, 7):
        rest_over_y(r)
    word_2()

    for i in range(NL):
        rows = rows_of(i)
        for d in range(2):
            arrived(ring.at[d, 0, i], y_recv.at[d, 0, i])
        total = terms[0, rows, :].astype(F32) + ring[0, 0, i].astype(F32) + ring[1, 0, i].astype(F32)
        if i < NL - 1:
            terms[0, rows, :] = total.astype(BF)
            send(terms.at[0, rows, :], ring_z.at[i], z_send.at[i], z_recv.at[i], {"zl": z_rel(i)})
    for copy in prompt_copies:
        copy.wait()
    for i in range(NL - 1):
        send(own_prompts, prompts.at[zl], p_send.at[i], p_recv.at[i], {"zl": z_rel(i)})
    prompts[zl] = own_prompts[...]
    word_3()
    for copy in state_copies:
        copy.wait()

    def update(at, grad):
        new_one = 0.9 * state[1, at] + 0.1 * grad
        new_two = 0.999 * state[2, at] + 0.001 * grad * grad
        first = new_one / (1.0 - 0.9**50)
        second = new_two / (1.0 - 0.999**50)
        old = state[0, at]
        new_master = old - 0.003 * (first / (jnp.sqrt(second) + 1e-08) + 0.01 * old)
        weight[0, at] = new_master.astype(BF)
        new_state[0, at] = new_master
        new_state[1, at] = new_one
        new_state[2, at] = new_two

    grad = rest_total(0)
    for r in (4, 3, 5, 2, 6, 1, 7):
        arrived(rest_y.at[r], ry_recv.at[r])
        grad = grad + rest_y[r].astype(F32)
    update(slice(FIRST_Y, ROWS), grad)
    grad = total
    for i in range(NL - 1):
        arrived(ring_z.at[i], z_recv.at[i])
        grad = grad + ring_z[i].astype(F32)
    update(slice(0, FIRST_Y), grad)

    def piece(place, n):
        return weight.at[place, pl.ds(*PIECE[n])]

    def held(d, s):
        return SLOT[(NY - step[d] * s) % NY]

    def pass_on(s, n, d, hops=1):
        send(
            piece(held(d, s - 1), n), piece(held(d, s - 2 + hops + 1), n), w_send.at[d, s - 2 + hops, n],
            w_recv.at[d, s - 2 + hops, n], {"y": lax.rem(y + hops * step[d], NY)},
        )

    def landed(s, n, d):
        arrived(piece(held(d, s), n), w_recv.at[d, s - 1, n])

    x_order = (2, 1, 3, 0)

    def project(g, core):
        lhs = [prompts[2 * core + n, lax.rem(x + far_x, NX)].reshape(SUB, COLS) for far_x in x_order for n in range(2)]
        rhs = weight[4 * g : 4 * g + 4].reshape(OUTS, COLS)
        return lax.dot_general(
            jnp.concatenate(lhs, axis=0), rhs, (((1,), (1,)), ((), ())), preferred_element_type=F32
        )

    def project_all(g):
        theirs = project(g, 1 - c)
        for i in range(NX):
            core_out[g, i] = theirs[i * 2 * SUB : (i + 1) * 2 * SUB].astype(BF)
            send(core_out.at[g, i], core_in.at[g, i], c_send.at[g, i], c_recv.at[g, i], {"c": 1 - c})
        own_part[g] = project(g, c).reshape(NX, 2 * SUB, OUTS)

    x_dir = (1, NX - 1)

    def part_sum(g, i, n, h):
        rows = slice(n * SUB + h * 16, n * SUB + (h + 1) * 16)
        return own_part[g, i, rows, :] + core_in[g, i, rows, :].astype(F32)

    def x_send_to(g, d, i, n, k, h):
        send(
            x_out.at[g, i, n, h], x_in.at[g, d, k, n, h], x_send.at[g, d, k, n, h], x_recv.at[g, d, k, n, h],
            {"x": lax.rem(x + x_dir[d], NX)},
        )

    def far(g, d, h):
        x_out[g, 0, d, h] = part_sum(g, 0, d, h).astype(BF)
        x_send_to(g, d, 0, d, 1, h)

    def near(g, d, n, h):
        total = part_sum(g, 1 + d, n, h)
        if n == d:
            arrived(x_in.at[g, d, 1, n, h], x_recv.at[g, d, 1, n, h])
            total = total + x_in[g, d, 1, n, h].astype(F32)
        x_out[g, 1 + d, n, h] = total.astype(BF)
        x_send_to(g, d, 1 + d, n, 0, h)

    def x_first(g):
        arrived(core_in.at[g, 0], c_recv.at[g, 0])
        for h in range(NH):
            for d in range(2):
                far(g, d, h)
        for d in range(2):
            arrived(core_in.at[g, 1 + d], c_recv.at[g, 1 + d])
        for h in range(NH):
            for d in range(2):
                near(g, d, 1 - d, h)

    def x_second(g):
        for h in range(NH):
            for d in range(2):
                near(g, d, d, h)
        arrived(core_in.at[g, 3], c_recv.at[g, 3])

    def over_z(g):
        for h in range(NH):
            for n in range(2):
                total = part_sum(g, 3, n, h)
                for d in range(2):
                    arrived(x_in.at[g, d, 0, n, h], x_recv.at[g, d, 0, n, h])
                    total = total + x_in[g, d, 0, n, h].astype(F32)
                z_out[g, n, h] = total.reshape(NC, 8, OUTS).astype(BF)
                for core in range(NC):
                    stays = jnp.logical_and(me == h * NL + 2 * c + n, c == core)

                    @pl.when(stays)
                    def _():
                        pltpu.make_async_copy(z_out.at[g, n, h, core], z_in.at[g, me], f_recv.at[g, me]).start()

                    @pl.when(jnp.logical_not(stays))
                    def _():
                        go(
                            z_out.at[g, n, h, core], z_in.at[g, me], f_send.at[g, n, h, core], f_recv.at[g, me],
                            {"zh": h, "zl": 2 * c + n, "c": core},
                        )

    for n in range(4):
        for d in range(2):
            pass_on(1, n, d)
    state_copy = pltpu.make_async_copy(new_state, state_out, store_sem)
    state_copy.start()
    for n in range(4):
        for d in range(2):
            landed(1, n, d)
            pass_on(2, n, d)
    for n in range(4):
        for d in range(2):
            landed(2, n, d)
            if n // 2 == d:
                pass_on(3, n, d, 2)
            pass_on(3, n, d)
    word_4()
    for i in range(NL - 1):
        arrived(prompts.at[0], p_recv.at[i])
    project_all(0)
    x_first(0)
    for n in range(4):
        for d in range(2):
            landed(3, n, d)
            if n // 2 == d:
                landed(4, n, d)
    word_5()
    project_all(1)
    x_second(0)
    x_first(1)
    over_z(0)
    x_second(1)
    over_z(1)

    for copy in sent:
        copy.wait_send()
    for g in range(2):
        for n in range(2):
            for h in range(NH):
                for core in range(NC):

                    @pl.when(jnp.logical_or(me != h * NL + 2 * c + n, c != core))
                    def _():
                        part = z_out.at[g, n, h, core]
                        pltpu.make_async_copy(part, part, f_send.at[g, n, h, core]).wait()

        for source in range(NZ):
            arrived(z_in.at[g, source], f_recv.at[g, source])
    state_copy.wait()


def finish(
    state, z_in, master_out, one_out, two_out, proj_out, held, parts, proj, read_sem, in_sem, out_sem
):
    y = lax.axis_index("y")
    read = pltpu.make_async_copy(z_in, parts, read_sem)
    read.start()
    outs = (master_out, one_out, two_out)
    reads = [pltpu.make_async_copy(state.at[i], held.at[i], in_sem.at[i]) for i in range(3)]
    writes = [pltpu.make_async_copy(held.at[i], outs[i], out_sem.at[i]) for i in range(3)]
    for copy in reads:
        copy.start()
    read.wait()
    for g in range(2):
        sums = []
        for n in range(NL):
            terms = [parts[g, h * NL + n].astype(F32) for h in range(NH)]
            sums.append(terms[0] + terms[1] + terms[2])
        for j in range(4):
            block = jnp.concatenate([part[:, j * ROWS : (j + 1) * ROWS] for part in sums], axis=1)
            far_y = lax.rem(y + PLACE[4 * g + j], NY)
            proj[:, pl.ds(pl.multiple_of(far_y * 640, 640), 640)] = block.astype(BF)
    last = pltpu.make_async_copy(proj, proj_out, out_sem.at[3])
    last.start()
    for copy, write in zip(reads, writes):
        copy.wait()
        write.start()
    for copy in writes:
        copy.wait()
    last.wait()


def local(activations, cotangent, master, moment_one, moment_two, prompts):
    any_space = pl.BlockSpec(memory_space=pl.ANY)
    dma = pltpu.SemaphoreType.DMA
    state, z_in = pl.pallas_call(
        kernel,
        out_shape=(jax.ShapeDtypeStruct((3, ROWS, COLS), F32), jax.ShapeDtypeStruct((2, NZ, 8, OUTS), BF)),
        in_specs=[any_space] * 6,
        out_specs=[any_space] * 2,
        scratch_shapes=[
            pltpu.VMEM((512, COLS), BF),
            pltpu.VMEM((NY, 512, 640), BF),
            pltpu.VMEM((3, ROWS, COLS), F32),
            pltpu.VMEM((3, ROWS, COLS), F32),
            pltpu.VMEM((NX, NH, 16, COLS), BF),
            pltpu.VMEM((NL, NX, NH, 16, COLS), BF),
            pltpu.VMEM((NY, 640, COLS), BF),
            pltpu.VMEM((2, 4, NL, FIRST_Y, COLS), BF),
            pltpu.VMEM((NL - 1, FIRST_Y, COLS), BF),
            pltpu.VMEM((NY, NL - 1, REST, COLS), BF),
            pltpu.VMEM((NY, REST, COLS), BF),
            pltpu.VMEM((NY, REST, COLS), BF),
            pltpu.VMEM((NY, ROWS, COLS), BF),
            pltpu.VMEM((2, NX, 2 * SUB, OUTS), F32),
            pltpu.VMEM((2, NX, 2 * SUB, OUTS), BF),
            pltpu.VMEM((2, NX, 2 * SUB, OUTS), BF),
            pltpu.VMEM((2, 3, 2, NH, 16, OUTS), BF),
            pltpu.VMEM((2, 2, 2, 2, NH, 16, OUTS), BF),
            pltpu.VMEM((2, 2, NH, NC, 8, OUTS), BF),
            dma((8,)), dma((NY,)), dma(()),
            dma((3,)), dma((3,)),
            dma((2, 5, NL)), dma((2, 4, NL)),
            dma((3,)), dma((3,)),
            dma((NY, 3)), dma((NY, 3)),
            dma((NY,)), dma((NY,)),
            dma((2, 4, 4)), dma((2, 4, 4)),
            dma((2, NX)), dma((2, NX)),
            dma((2, 2, 2, 2, NH)), dma((2, 2, 2, 2, NH)),
            dma((2, 2, NH, NC)), dma((2, NZ)),
            *[pltpu.SemaphoreType.REGULAR] * 4,
        ],
        compiler_params=pltpu.CompilerParams(collective_id=0, has_side_effects=True),
        name="step",
    )(activations, cotangent, master, moment_one, moment_two, prompts.reshape(NH, NX, 16, COLS))
    weight_shape = jax.ShapeDtypeStruct((ROWS, COLS), F32)
    return pl.pallas_call(
        finish,
        out_shape=(weight_shape, weight_shape, weight_shape, jax.ShapeDtypeStruct((8, 5120), BF)),
        in_specs=[any_space] * 2,
        out_specs=[any_space] * 4,
        scratch_shapes=[
            pltpu.VMEM((3, ROWS, COLS), F32), pltpu.VMEM((2, NZ, 8, OUTS), BF), pltpu.VMEM((8, 5120), BF),
            dma(()), dma((3,)), dma((4,)),
        ],
        name="finish",
    )(state, z_in)


def solution(mesh):
    torus = Mesh(mesh.devices.reshape(NY, NL, NH, NX, NC), AXES)
    dp, tensor = ("y", "zl"), ("zh", "x", "c")
    both = P(dp, tensor)
    in_specs = (both, P(dp, None), both, both, both, both)
    out_specs = (both, both, both, P(dp + tensor, None))
    return jax.shard_map(local, mesh=torus, in_specs=in_specs, out_specs=out_specs, check_vma=False)
```

```python
import jax
import jax.numpy as jnp
from jax import lax
from jax.experimental import pallas as pl
from jax.experimental.pallas import tpu as pltpu
from jax.sharding import Mesh
from jax.sharding import PartitionSpec as P

AXES = ("y", "zl", "zh", "x", "c")
NY, NL, NH, NX, NC = 8, 4, 3, 4, 2
NZ = NL * NH
BF = jnp.bfloat16
F32 = jnp.float32

ROWS = 160
FIRST_Y = 112
REST = ROWS - FIRST_Y
HALF = ((0, 64), (64, 48))
COLS = 256
OUTS = 4 * ROWS
SUB = NH * 16
PLACE = (0, 1, 7, 2, 6, 3, 5, 4)
SLOT = tuple(PLACE.index(r) for r in range(NY))
PIECE = ((0, 48), (48, 32), (80, 48), (128, 32))
MESH = pl.DeviceIdType.MESH


def kernel(
    act_hbm, cot_hbm, master_hbm, one_hbm, two_hbm, prompts_hbm,
    state_out, z_in,
    act, cot, state, new_state, own_prompts, prompts, terms, ring, ring_z, rest_z, rest_y, rest_sum,
    weight, own_part, core_out, core_in, x_out, x_in, z_out,
    load_sem, cot_sem, store_sem, p_send, p_recv, y_send, y_recv, z_send, z_recv,
    rz_send, rz_recv, ry_send, ry_recv,
    w_send, w_recv, c_send, c_recv, x_send, x_recv, f_send, f_recv,
    up_edge, up_group, down_edge, down_group,
):
    y, zl, zh, x, c = (lax.axis_index(axis) for axis in AXES)
    sent = []

    def go(src, dst, send_sem, recv_sem, to):
        copy = pltpu.make_async_remote_copy(
            src_ref=src, dst_ref=dst, send_sem=send_sem, recv_sem=recv_sem,
            device_id=to, device_id_type=MESH,
        )
        copy.start()
        return copy

    def send(src, dst, send_sem, recv_sem, to):
        sent.append(go(src, dst, send_sem, recv_sem, to))

    def arrived(dst, recv_sem):
        pltpu.make_async_copy(dst, dst, recv_sem).wait()

    def cot_copy(r):
        first = pl.multiple_of(lax.rem(y + r, NY) * 640, 640)
        return pltpu.make_async_copy(cot_hbm.at[:, pl.ds(first, 640)], cot.at[r], cot_sem.at[r])

    act_copy = pltpu.make_async_copy(act_hbm, act, load_sem.at[0])
    act_copy.start()
    for r in (4, 3, 5, 2, 6, 1, 7, 0):
        cot_copy(r).start()
    prompt_copies = [
        pltpu.make_async_copy(prompts_hbm.at[:, i], own_prompts.at[i], load_sem.at[1 + i]) for i in range(NX)
    ]
    state_copies = [
        pltpu.make_async_copy(ref, state.at[i], load_sem.at[5 + i])
        for i, ref in enumerate((master_hbm, one_hbm, two_hbm))
    ]
    for copy in prompt_copies + state_copies:
        copy.start()

    barrier = pltpu.get_barrier_semaphore()
    peers = [{"y": lax.rem(y + i, NY)} for i in range(1, NY)]
    peers += [{"zl": lax.rem(zl + i, NL)} for i in range(1, NL)]
    peers += [{"x": lax.rem(x + 1, NX)}, {"x": lax.rem(x + NX - 1, NX)}, {"c": 1 - c}]
    for peer in peers:
        pl.semaphore_signal(barrier, inc=1, device_id=peer, device_id_type=MESH)
    me = zh * NL + zl
    lower_edge = jnp.logical_and(zl == 0, zh > 0)
    upper_edge = jnp.logical_and(zl == NL - 1, zh < NH - 1)

    def tell(semaphore, peer):
        pl.semaphore_signal(semaphore, inc=1, device_id=peer, device_id_type=MESH)

    pl.when(lower_edge)(lambda: tell(barrier, {"zh": zh - 1, "zl": NL - 1}))
    pl.when(upper_edge)(lambda: tell(barrier, {"zh": zh + 1, "zl": 0}))

    def at(h, n):
        return jnp.logical_and(zh == h, zl == n)

    def tell_group(semaphore):
        for i in range(1, NL):
            tell(semaphore, {"zl": lax.rem(zl + i, NL)})

    def word_1():
        pl.when(at(0, 3))(lambda: tell(up_edge, {"zh": 1, "zl": 0}))
        pl.when(at(2, 0))(lambda: tell(down_edge, {"zh": 1, "zl": 3}))

    def hear_and_tell_group(h, n, edge, group):
        @pl.when(at(h, n))
        def _():
            pl.semaphore_wait(edge, 1)
            tell_group(group)

    def word_2():
        hear_and_tell_group(1, 0, up_edge, up_group)
        hear_and_tell_group(1, 3, down_edge, down_group)

    def word_3():
        @pl.when(at(1, 3))
        def _():
            pl.semaphore_wait(up_group, 1)
            tell(up_edge, {"zh": 2, "zl": 0})

        @pl.when(at(1, 0))
        def _():
            pl.semaphore_wait(down_group, 1)
            tell(down_edge, {"zh": 0, "zl": 3})

    def word_4():
        hear_and_tell_group(2, 0, up_edge, up_group)
        hear_and_tell_group(0, 3, down_edge, down_group)

    def word_5():
        middle = jnp.logical_and(zh == 1, jnp.logical_or(zl == 1, zl == 2))
        below = jnp.logical_or(middle, jnp.logical_and(zh == 2, zl != 0))
        above = jnp.logical_or(middle, jnp.logical_and(zh == 0, zl != 3))
        pl.when(below)(lambda: pl.semaphore_wait(up_group, 1))
        pl.when(above)(lambda: pl.semaphore_wait(down_group, 1))

    def term(r):
        cot_copy(r).wait()
        for b in range(5):
            block = lax.dot_general(
                cot[r, :, b * 128 : (b + 1) * 128], act[...],
                (((0,), (0,)), ((), ())), preferred_element_type=F32,
            )
            terms[r, b * 128 : (b + 1) * 128, :] = block.astype(BF)

    def z_rel(i):
        if i == NL - 1:
            return zl
        down = NL - 1 - i - (NL - 1 - i <= zl).astype(jnp.int32)
        up = i + (i >= zl).astype(jnp.int32)
        return down + zl // 2 * (up - down)

    def slot(i):
        return lax.rem(zl - z_rel(i) + NL, NL) - 1

    def rows_of(i, first=0, size=FIRST_Y):
        return pl.ds(pl.multiple_of(z_rel(i) * ROWS + first, 16), size)

    def rest_of(i):
        return pl.ds(pl.multiple_of(z_rel(i) * ROWS + FIRST_Y, 16), REST)

    def rest_over_z(r):
        for i in range(NL - 1):
            send(
                terms.at[r, rest_of(i), :], rest_z.at[r, slot(i)], rz_send.at[r, i], rz_recv.at[r, slot(i)],
                {"zl": z_rel(i)},
            )

    def rest_total(r):
        total = terms[r, rest_of(NL - 1), :].astype(F32)
        for i in range(NL - 1):
            arrived(rest_z.at[r, i], rz_recv.at[r, i])
            total = total + rest_z[r, i].astype(F32)
        return total

    def rest_over_y(r):
        rest_sum[r] = rest_total(r).astype(BF)
        send(rest_sum.at[r], rest_y.at[r], ry_send.at[r], ry_recv.at[r], {"y": lax.rem(y + r, NY)})

    act_copy.wait()
    term(4)
    pl.semaphore_wait(barrier, len(peers) + lower_edge.astype(jnp.int32) + upper_edge.astype(jnp.int32))

    step = (1, NY - 1)

    def chain(k):
        for i in range(NL):
            for d in range(2):
                r = (step[d] * k) % NY
                half = HALF[d]
                if k < 4:
                    first, size = half if k == 3 else (0, FIRST_Y)
                    got, to = rows_of(i, first, size), pl.ds(first, size)
                    arrived(ring.at[d, k, i, to], y_recv.at[d, k, i])
                    total = terms[r, got, :].astype(F32) + ring[d, k, i, to].astype(F32)
                    terms[r, got, :] = total.astype(BF)
                first, size = half if k == 4 else (0, FIRST_Y)
                send(
                    terms.at[r, rows_of(i, first, size), :], ring.at[d, k - 1, i, pl.ds(first, size)],
                    y_send.at[d, k, i], y_recv.at[d, k - 1, i], {"y": lax.rem(y + step[d], NY)},
                )

    chain(4)
    rest_over_z(4)
    for r in (3, 5):
        term(r)
        rest_over_z(r)
    chain(3)
    for r in (2, 6):
        term(r)
        rest_over_z(r)
    rest_over_y(4)
    word_1()
    chain(2)
    for r in (1, 7, 0):
        term(r)
        rest_over_z(r)
    for r in (3, 5):
        rest_over_y(r)
    chain(1)
    for r in (2, 6, 1, 7):
        rest_over_y(r)
    word_2()

    for i in range(NL):
        rows = rows_of(i)
        for d in range(2):
            arrived(ring.at[d, 0, i], y_recv.at[d, 0, i])
        total = terms[0, rows, :].astype(F32) + ring[0, 0, i].astype(F32) + ring[1, 0, i].astype(F32)
        if i < NL - 1:
            terms[0, rows, :] = total.astype(BF)
            send(terms.at[0, rows, :], ring_z.at[slot(i)], z_send.at[i], z_recv.at[slot(i)], {"zl": z_rel(i)})
    for copy in prompt_copies:
        copy.wait()
    for i in range(NL - 1):
        send(own_prompts, prompts.at[zl], p_send.at[i], p_recv.at[slot(i)], {"zl": z_rel(i)})
    prompts[zl] = own_prompts[...]
    word_3()
    for copy in state_copies:
        copy.wait()

    def update(at, grad):
        new_one = 0.9 * state[1, at] + 0.1 * grad
        new_two = 0.999 * state[2, at] + 0.001 * grad * grad
        first = new_one / (1.0 - 0.9**50)
        second = new_two / (1.0 - 0.999**50)
        old = state[0, at]
        new_master = old - 0.003 * (first / (jnp.sqrt(second) + 1e-08) + 0.01 * old)
        weight[0, at] = new_master.astype(BF)
        new_state[0, at] = new_master
        new_state[1, at] = new_one
        new_state[2, at] = new_two

    grad = rest_total(0)
    for r in (4, 3, 5, 2, 6, 1, 7):
        arrived(rest_y.at[r], ry_recv.at[r])
        grad = grad + rest_y[r].astype(F32)
    update(slice(FIRST_Y, ROWS), grad)
    grad = total
    for i in range(NL - 1):
        arrived(ring_z.at[i], z_recv.at[i])
        grad = grad + ring_z[i].astype(F32)
    update(slice(0, FIRST_Y), grad)

    def piece(place, n):
        return weight.at[place, pl.ds(*PIECE[n])]

    def held(d, s):
        return SLOT[(NY - step[d] * s) % NY]

    def pass_on(s, n, d, hops=1):
        send(
            piece(held(d, s - 1), n), piece(held(d, s - 2 + hops + 1), n), w_send.at[d, s - 2 + hops, n],
            w_recv.at[d, s - 2 + hops, n], {"y": lax.rem(y + hops * step[d], NY)},
        )

    def landed(s, n, d):
        arrived(piece(held(d, s), n), w_recv.at[d, s - 1, n])

    x_order = (2, 1, 3, 0)

    def project(g, core):
        lhs = [prompts[2 * core + n, lax.rem(x + far_x, NX)].reshape(SUB, COLS) for far_x in x_order for n in range(2)]
        rhs = weight[4 * g : 4 * g + 4].reshape(OUTS, COLS)
        return lax.dot_general(
            jnp.concatenate(lhs, axis=0), rhs, (((1,), (1,)), ((), ())), preferred_element_type=F32
        )

    def project_all(g):
        theirs = project(g, 1 - c)
        for i in range(NX):
            core_out[g, i] = theirs[i * 2 * SUB : (i + 1) * 2 * SUB].astype(BF)
            send(core_out.at[g, i], core_in.at[g, i], c_send.at[g, i], c_recv.at[g, i], {"c": 1 - c})
        own_part[g] = project(g, c).reshape(NX, 2 * SUB, OUTS)

    x_dir = (1, NX - 1)

    def part_sum(g, i, n, h):
        rows = slice(n * SUB + h * 16, n * SUB + (h + 1) * 16)
        return own_part[g, i, rows, :] + core_in[g, i, rows, :].astype(F32)

    def x_send_to(g, d, i, n, k, h):
        send(
            x_out.at[g, i, n, h], x_in.at[g, d, k, n, h], x_send.at[g, d, k, n, h], x_recv.at[g, d, k, n, h],
            {"x": lax.rem(x + x_dir[d], NX)},
        )

    def far(g, d, h):
        x_out[g, 0, d, h] = part_sum(g, 0, d, h).astype(BF)
        x_send_to(g, d, 0, d, 1, h)

    def near(g, d, n, h):
        total = part_sum(g, 1 + d, n, h)
        if n == d:
            arrived(x_in.at[g, d, 1, n, h], x_recv.at[g, d, 1, n, h])
            total = total + x_in[g, d, 1, n, h].astype(F32)
        x_out[g, 1 + d, n, h] = total.astype(BF)
        x_send_to(g, d, 1 + d, n, 0, h)

    def x_first(g):
        arrived(core_in.at[g, 0], c_recv.at[g, 0])
        for h in range(NH):
            for d in range(2):
                far(g, d, h)
        for d in range(2):
            arrived(core_in.at[g, 1 + d], c_recv.at[g, 1 + d])
        for h in range(NH):
            for d in range(2):
                near(g, d, 1 - d, h)

    def x_second(g):
        for h in range(NH):
            for d in range(2):
                near(g, d, d, h)
        arrived(core_in.at[g, 3], c_recv.at[g, 3])

    def over_z(g):
        for h in range(NH):
            for n in range(2):
                total = part_sum(g, 3, n, h)
                for d in range(2):
                    arrived(x_in.at[g, d, 0, n, h], x_recv.at[g, d, 0, n, h])
                    total = total + x_in[g, d, 0, n, h].astype(F32)
                z_out[g, n, h] = total.reshape(NC, 8, OUTS).astype(BF)
                for core in range(NC):
                    stays = jnp.logical_and(me == h * NL + 2 * c + n, c == core)

                    @pl.when(stays)
                    def _():
                        pltpu.make_async_copy(z_out.at[g, n, h, core], z_in.at[g, me], f_recv.at[g, me]).start()

                    @pl.when(jnp.logical_not(stays))
                    def _():
                        go(
                            z_out.at[g, n, h, core], z_in.at[g, me], f_send.at[g, n, h, core], f_recv.at[g, me],
                            {"zh": h, "zl": 2 * c + n, "c": core},
                        )

    for n in range(4):
        for d in range(2):
            pass_on(1, n, d)
    state_copy = pltpu.make_async_copy(new_state, state_out, store_sem)
    state_copy.start()
    for n in range(4):
        for d in range(2):
            landed(1, n, d)
            pass_on(2, n, d)
    for n in range(4):
        for d in range(2):
            landed(2, n, d)
            if n // 2 == d:
                pass_on(3, n, d, 2)
            pass_on(3, n, d)
    word_4()
    for i in range(NL - 1):
        arrived(prompts.at[0], p_recv.at[i])
    project_all(0)
    x_first(0)
    for n in range(4):
        for d in range(2):
            landed(3, n, d)
            if n // 2 == d:
                landed(4, n, d)
    word_5()
    project_all(1)
    x_second(0)
    x_first(1)
    over_z(0)
    x_second(1)
    over_z(1)

    for copy in sent:
        copy.wait_send()
    for g in range(2):
        for n in range(2):
            for h in range(NH):
                for core in range(NC):

                    @pl.when(jnp.logical_or(me != h * NL + 2 * c + n, c != core))
                    def _():
                        part = z_out.at[g, n, h, core]
                        pltpu.make_async_copy(part, part, f_send.at[g, n, h, core]).wait()

        for source in range(NZ):
            arrived(z_in.at[g, source], f_recv.at[g, source])
    state_copy.wait()


def finish(
    state, z_in, master_out, one_out, two_out, proj_out, held, parts, proj, read_sem, in_sem, out_sem
):
    y = lax.axis_index("y")
    read = pltpu.make_async_copy(z_in, parts, read_sem)
    read.start()
    outs = (master_out, one_out, two_out)
    reads = [pltpu.make_async_copy(state.at[i], held.at[i], in_sem.at[i]) for i in range(3)]
    writes = [pltpu.make_async_copy(held.at[i], outs[i], out_sem.at[i]) for i in range(3)]
    for copy in reads:
        copy.start()
    read.wait()
    for g in range(2):
        sums = []
        for n in range(NL):
            terms = [parts[g, h * NL + n].astype(F32) for h in range(NH)]
            sums.append(terms[0] + terms[1] + terms[2])
        for j in range(4):
            block = jnp.concatenate([part[:, j * ROWS : (j + 1) * ROWS] for part in sums], axis=1)
            far_y = lax.rem(y + PLACE[4 * g + j], NY)
            proj[:, pl.ds(pl.multiple_of(far_y * 640, 640), 640)] = block.astype(BF)
    last = pltpu.make_async_copy(proj, proj_out, out_sem.at[3])
    last.start()
    for copy, write in zip(reads, writes):
        copy.wait()
        write.start()
    for copy in writes:
        copy.wait()
    last.wait()


def local(activations, cotangent, master, moment_one, moment_two, prompts):
    any_space = pl.BlockSpec(memory_space=pl.ANY)
    dma = pltpu.SemaphoreType.DMA
    state, z_in = pl.pallas_call(
        kernel,
        out_shape=(jax.ShapeDtypeStruct((3, ROWS, COLS), F32), jax.ShapeDtypeStruct((2, NZ, 8, OUTS), BF)),
        in_specs=[any_space] * 6,
        out_specs=[any_space] * 2,
        scratch_shapes=[
            pltpu.VMEM((512, COLS), BF),
            pltpu.VMEM((NY, 512, 640), BF),
            pltpu.VMEM((3, ROWS, COLS), F32),
            pltpu.VMEM((3, ROWS, COLS), F32),
            pltpu.VMEM((NX, NH, 16, COLS), BF),
            pltpu.VMEM((NL, NX, NH, 16, COLS), BF),
            pltpu.VMEM((NY, 640, COLS), BF),
            pltpu.VMEM((2, 4, NL, FIRST_Y, COLS), BF),
            pltpu.VMEM((NL - 1, FIRST_Y, COLS), BF),
            pltpu.VMEM((NY, NL - 1, REST, COLS), BF),
            pltpu.VMEM((NY, REST, COLS), BF),
            pltpu.VMEM((NY, REST, COLS), BF),
            pltpu.VMEM((NY, ROWS, COLS), BF),
            pltpu.VMEM((2, NX, 2 * SUB, OUTS), F32),
            pltpu.VMEM((2, NX, 2 * SUB, OUTS), BF),
            pltpu.VMEM((2, NX, 2 * SUB, OUTS), BF),
            pltpu.VMEM((2, 3, 2, NH, 16, OUTS), BF),
            pltpu.VMEM((2, 2, 2, 2, NH, 16, OUTS), BF),
            pltpu.VMEM((2, 2, NH, NC, 8, OUTS), BF),
            dma((8,)), dma((NY,)), dma(()),
            dma((3,)), dma((3,)),
            dma((2, 5, NL)), dma((2, 4, NL)),
            dma((3,)), dma((3,)),
            dma((NY, 3)), dma((NY, 3)),
            dma((NY,)), dma((NY,)),
            dma((2, 4, 4)), dma((2, 4, 4)),
            dma((2, NX)), dma((2, NX)),
            dma((2, 2, 2, 2, NH)), dma((2, 2, 2, 2, NH)),
            dma((2, 2, NH, NC)), dma((2, NZ)),
            *[pltpu.SemaphoreType.REGULAR] * 4,
        ],
        compiler_params=pltpu.CompilerParams(collective_id=0, has_side_effects=True),
        name="step",
    )(activations, cotangent, master, moment_one, moment_two, prompts.reshape(NH, NX, 16, COLS))
    weight_shape = jax.ShapeDtypeStruct((ROWS, COLS), F32)
    return pl.pallas_call(
        finish,
        out_shape=(weight_shape, weight_shape, weight_shape, jax.ShapeDtypeStruct((8, 5120), BF)),
        in_specs=[any_space] * 2,
        out_specs=[any_space] * 4,
        scratch_shapes=[
            pltpu.VMEM((3, ROWS, COLS), F32), pltpu.VMEM((2, NZ, 8, OUTS), BF), pltpu.VMEM((8, 5120), BF),
            dma(()), dma((3,)), dma((4,)),
        ],
        name="finish",
    )(state, z_in)


def solution(mesh):
    torus = Mesh(mesh.devices.reshape(NY, NL, NH, NX, NC), AXES)
    dp, tensor = ("y", "zl"), ("zh", "x", "c")
    both = P(dp, tensor)
    in_specs = (both, P(dp, None), both, both, both, both)
    out_specs = (both, both, both, P(dp + tensor, None))
    return jax.shard_map(local, mesh=torus, in_specs=in_specs, out_specs=out_specs, check_vma=False)
```
